32 devices in a mesh: dp: 1 (over z), ep: 32 (over y, x, core).
Axes of the slice: x: 4, y: 4, z: 1, core: 2. Of those that a mesh axis runs over, the one named last changes fastest.
The devices are a block of a 4x4x8 slice.
Arguments:
- hidden: bfloat16 [8192, 2048], P(('dp', 'ep'))
- norm_gain: bfloat16 [2048], replicated
- w_gate: bfloat16 [2048, 64], replicated
- w1_shared: bfloat16 [2048, 2816], replicated
- w3_shared: bfloat16 [2048, 2816], replicated
- w2_shared: bfloat16 [2816, 2048], replicated
- w1_experts: bfloat16 [64, 2048, 1408], P('ep')
- w3_experts: bfloat16 [64, 2048, 1408], P('ep')
- w2_experts: bfloat16 [64, 1408, 2048], P('ep')
- topk_ids: int32 [8192, 6], P(('dp', 'ep'))
Outputs:
- output: bfloat16 [8192, 2048], P(('dp', 'ep'))
All inputs are finite; a program needn't handle non-finite values.
Results may differ from the reference program's by a relative error of at most 0.00588174.
Values are sent between devices in bfloat16 or wider.
A program may use at most 768 MiB of HBM per device.

```python
import jax
import jax.numpy as jnp
from jax import lax

HIDDEN = 2048
EXPERTS = 64
EXPERT_FF = 1408
SHARED_FF = 2816
TOP_K = 6
TOKENS_DEV = 256
TOKENS = 8192
GROUPS = 8
TOP_GROUPS = 3
ROUTE_SCALE = 16
NORM_EPS = 1e-6
GROUP_SIZE = EXPERTS // GROUPS


def draw_routing(route_key):
    blocks = TOKENS // TOKENS_DEV
    half_block = TOKENS_DEV // 2
    key_hot, key_cycle, key_perm, key_score, key_pick = jax.random.split(route_key, 5)
    hot_group = jax.random.randint(key_hot, (blocks, 1, 1), 0, GROUPS)
    cycle_off = jax.random.randint(key_cycle, (blocks, 1, 1), 0, GROUPS - 1)
    perm_keys = jax.random.split(key_perm, blocks)
    rank_in = jax.vmap(lambda sub_key: jax.random.permutation(sub_key, TOKENS_DEV))(perm_keys)[:, :, None]
    first_set = (rank_in * (TOP_GROUPS - 1) + jnp.arange(TOP_GROUPS - 1) + cycle_off) % (GROUPS - 1)
    first_groups = jnp.concatenate([jnp.broadcast_to(hot_group, (blocks, TOKENS_DEV, 1)), (hot_group + 1 + first_set) % GROUPS], axis=2)
    second_set = (rank_in * TOP_GROUPS + jnp.arange(TOP_GROUPS) + cycle_off) % (GROUPS - 1)
    second_groups = (hot_group + 1 + second_set) % GROUPS
    chosen = jnp.where(rank_in < half_block, first_groups, second_groups).reshape(TOKENS, TOP_GROUPS)
    scores = jax.random.randint(key_score, (TOKENS, TOP_GROUPS, GROUP_SIZE), 0, 2 ** 19) * 512
    scores = scores + jnp.arange(TOP_GROUPS * GROUP_SIZE).reshape(TOP_GROUPS, GROUP_SIZE)
    pick_idx = jax.random.randint(key_pick, (TOKENS, TOP_GROUPS, 1), 0, GROUP_SIZE)
    scores = scores + jnp.where(jnp.arange(GROUP_SIZE) == pick_idx, 2 ** 29, 0)
    cand_idx = lax.top_k(scores.reshape(TOKENS, TOP_GROUPS * GROUP_SIZE), TOP_K)[1]
    group_of = jnp.take_along_axis(chosen, cand_idx // GROUP_SIZE, axis=1)
    return (group_of * GROUP_SIZE + cand_idx % GROUP_SIZE).astype(jnp.int32)


def normal_bf16(sub_key, shape_in, scale_by):
    return (scale_by * jax.random.normal(sub_key, shape_in, jnp.float32)).astype(jnp.bfloat16)


def setup_inputs(seed: int = 0, part: int = 0) -> dict:
    part_key = jax.random.fold_in(jax.random.key(seed), part)
    weight_keys = jax.random.split(jax.random.key(seed + 1), 8)
    hidden = normal_bf16(jax.random.fold_in(part_key, 1), (TOKENS, HIDDEN), 0.5)
    norm_gain = (1.0 + 0.2 * jax.random.normal(weight_keys[0], (HIDDEN,), jnp.float32)).astype(jnp.bfloat16)
    w_gate = normal_bf16(weight_keys[1], (HIDDEN, EXPERTS), HIDDEN ** -0.5)
    w1_shared = normal_bf16(weight_keys[2], (HIDDEN, SHARED_FF), HIDDEN ** -0.5)
    w3_shared = normal_bf16(weight_keys[3], (HIDDEN, SHARED_FF), HIDDEN ** -0.5)
    w2_shared = normal_bf16(weight_keys[4], (SHARED_FF, HIDDEN), SHARED_FF ** -0.5)
    w1_experts = normal_bf16(weight_keys[5], (EXPERTS, HIDDEN, EXPERT_FF), HIDDEN ** -0.5)
    w3_experts = normal_bf16(weight_keys[6], (EXPERTS, HIDDEN, EXPERT_FF), HIDDEN ** -0.5)
    w2_experts = normal_bf16(weight_keys[7], (EXPERTS, EXPERT_FF, HIDDEN), EXPERT_FF ** -0.5)
    topk_ids = draw_routing(jax.random.fold_in(part_key, 2))
    return dict(hidden=hidden, norm_gain=norm_gain, w_gate=w_gate, w1_shared=w1_shared, w3_shared=w3_shared, w2_shared=w2_shared, w1_experts=w1_experts, w3_experts=w3_experts, w2_experts=w2_experts, topk_ids=topk_ids)


def rms_norm(hidden, norm_gain):
    rows_f = hidden.astype(jnp.float32)
    inv_rms = lax.rsqrt(jnp.mean(rows_f * rows_f, axis=-1, keepdims=True) + NORM_EPS)
    return (rows_f * inv_rms * norm_gain.astype(jnp.float32)).astype(jnp.bfloat16)


def swiglu(rows_in, w_up, w_lin, w_down):
    gate_act = jnp.dot(rows_in, w_up, preferred_element_type=jnp.float32)
    lin_act = jnp.dot(rows_in, w_lin, preferred_element_type=jnp.float32)
    inner_act = (jax.nn.silu(gate_act) * lin_act).astype(jnp.bfloat16)
    return jnp.dot(inner_act, w_down, preferred_element_type=jnp.float32).astype(jnp.bfloat16)


def reference(hidden, norm_gain, w_gate, w1_shared, w3_shared, w2_shared, w1_experts, w3_experts, w2_experts, topk_ids):
    normed = rms_norm(hidden, norm_gain)
    gate_probs = jax.nn.softmax(jnp.dot(normed, w_gate, preferred_element_type=jnp.float32), axis=-1)
    gate_wts = ROUTE_SCALE * jnp.take_along_axis(gate_probs, topk_ids, axis=1)
    shared_out = swiglu(normed, w1_shared, w3_shared, w2_shared)

    def expert_step(routed_acc, expert_in):
        w_up, w_lin, w_down, expert_id = expert_in
        column = jnp.sum(jnp.where(topk_ids == expert_id, gate_wts, 0.0), axis=1)
        expert_out = swiglu(normed, w_up, w_lin, w_down)
        return routed_acc + column[:, None] * expert_out.astype(jnp.float32), None

    routed = lax.scan(expert_step, jnp.zeros(hidden.shape, jnp.float32), (w1_experts, w3_experts, w2_experts, jnp.arange(EXPERTS)))[0]
    return (hidden.astype(jnp.float32) + shared_out.astype(jnp.float32) + routed).astype(jnp.bfloat16)
```

```python
import functools

import jax
import jax.numpy as jnp
from jax import lax
from jax.experimental import pallas as pl
from jax.experimental.pallas import tpu as pltpu
from jax.sharding import PartitionSpec as P

ROUTE_SCALE = 16
NORM_EPS = 1e-6
QUAD = 4
MESH = pl.DeviceIdType.MESH


def rms_norm(hidden, norm_gain):
    rows_f = hidden.astype(jnp.float32)
    inv_rms = lax.rsqrt(jnp.mean(rows_f * rows_f, axis=-1, keepdims=True) + NORM_EPS)
    return (rows_f * inv_rms * norm_gain.astype(jnp.float32)).astype(jnp.bfloat16)


def swiglu(rows_in, w_up, w_lin, w_down):
    gate_act = jnp.dot(rows_in, w_up, preferred_element_type=jnp.float32)
    lin_act = jnp.dot(rows_in, w_lin, preferred_element_type=jnp.float32)
    inner_act = (jax.nn.silu(gate_act) * lin_act).astype(jnp.bfloat16)
    return jnp.dot(inner_act, w_down, preferred_element_type=jnp.float32).astype(jnp.bfloat16)


def assign_slots(mask, cap_e):
    rows = mask.shape[-3]
    before = (jnp.arange(rows)[:, None] > jnp.arange(rows)[None, :]).astype(jnp.bfloat16)
    rank = jnp.einsum('ut,...tde->...ude', before, mask.astype(jnp.bfloat16), preferred_element_type=jnp.float32)
    total = jnp.sum(mask, axis=-3)
    count = jnp.minimum(total, cap_e)
    local = mask.shape[-1]
    later = (jnp.arange(local)[:, None] < jnp.arange(local)[None, :]).astype(jnp.float32)
    start = jnp.sum(count[..., :, None] * later, axis=-2)
    return rank, total, count, start


def moe_kernel(n, cap_e, cap, rows_ref, pick_ref, pack_ref, w1_ref, w3_ref, w2_ref, recv_ref,
               w1_v, w3_v, w2_v, row_v, x_v, h_v, y_v, stage_v, w_sem, row_sem, send_sem, recv_sem):
    side_n = n // 2
    side = next(s for s in range(1, side_n + 1) if s * s >= side_n)
    tiles = n // QUAD
    local, depth, inner = w1_ref.shape
    me = lax.axis_index('ep')
    core, col, line = me % 2, (me // 2) % side, me // (2 * side)

    def peer(k, q):
        turn = (k + 1) % (tiles // 2)
        dcore = 1 - k // (tiles // 2)
        to_col = (col + q) % side
        to_line = (line + q + turn) % side
        return (to_line * side + to_col) * 2 + (core + dcore) % 2

    loads = []
    for e in range(local):
        for j, (src, dst) in enumerate(((w1_ref, w1_v), (w3_ref, w3_v), (w2_ref, w2_v))):
            loads.append(pltpu.make_async_copy(src.at[e], dst.at[e], w_sem.at[3 * e + j]))

    def row_copy(k, q):
        return pltpu.make_async_copy(rows_ref.at[peer(k, q)], row_v.at[k % 2, q], row_sem.at[k % 2, q])

    def send_copy(k, q):
        return pltpu.make_async_remote_copy(
            src_ref=stage_v.at[k % 2, q], dst_ref=recv_ref.at[me],
            send_sem=send_sem.at[k % 2, q], recv_sem=recv_sem.at[k * QUAD + q],
            device_id={'ep': peer(k, q)}, device_id_type=MESH)

    def self_copy(k, q):
        return pltpu.make_async_copy(stage_v.at[k % 2, q], recv_ref.at[me], recv_sem.at[k * QUAD + q])

    for q in range(QUAD):
        row_copy(0, q).start()
    for load in loads:
        load.start()

    barrier = pltpu.get_barrier_semaphore()
    for off in range(1, n):
        pl.semaphore_signal(barrier, inc=1, device_id={'ep': (me + off) % n}, device_id_type=MESH)
    pl.semaphore_wait(barrier, n - 1)

    def columns(i, width):
        return pl.ds(pl.multiple_of(i * width, width), width)

    def tile(k, carry):
        slot = k % 2

        @pl.when(k + 1 < tiles)
        def _():
            for q in range(QUAD):
                row_copy(k + 1, q).start()

        for q in range(QUAD):
            row_copy(k, q).wait()
            width = min(512, depth)
            pick = pick_ref[peer(k, q)]

            def gather(i, carry):
                got = jnp.dot(pick, row_v[slot, q, :, columns(i, width)], preferred_element_type=jnp.float32)
                got = got.astype(jnp.bfloat16)
                for e in range(local):
                    x_v[e, q * cap_e:(q + 1) * cap_e, columns(i, width)] = got[e * cap_e:(e + 1) * cap_e]
                return carry

            lax.fori_loop(0, depth // width, gather, 0)

        for e in range(local):
            @pl.when(k == 0)
            def _():
                loads[3 * e].wait()
                loads[3 * e + 1].wait()

            def up_cols(at):
                rows_in = x_v[e]
                gate_act = jnp.dot(rows_in, w1_v[e, :, at], preferred_element_type=jnp.float32)
                lin_act = jnp.dot(rows_in, w3_v[e, :, at], preferred_element_type=jnp.float32)
                h_v[:, at] = (jax.nn.silu(gate_act) * lin_act).astype(jnp.bfloat16)

            def up(i, carry):
                up_cols(columns(i, 256))
                return carry

            lax.fori_loop(0, inner // 256, up, 0)
            if inner % 256:
                up_cols(pl.ds(inner - inner % 256, inner % 256))

            @pl.when(k == 0)
            def _():
                loads[3 * e + 2].wait()

            def down(i, carry):
                at = columns(i, 256)
                got = jnp.dot(h_v[...], w2_v[e, :, at], preferred_element_type=jnp.float32).astype(jnp.bfloat16)
                for q in range(QUAD):
                    y_v[q, e * cap_e:(e + 1) * cap_e, at] = got[q * cap_e:(q + 1) * cap_e]
                return carry

            lax.fori_loop(0, depth // 256, down, 0)

        @pl.when(k >= 2)
        def _():
            for q in range(QUAD):
                send_copy(k - 2, q).wait_send()

        for q in range(QUAD):
            width = min(512, depth)
            pack = pack_ref[peer(k, q)]

            def compact(i, carry):
                at = columns(i, width)
                got = jnp.dot(pack, y_v[q, :, at], preferred_element_type=jnp.float32)
                stage_v[slot, q, :, at] = got.astype(jnp.bfloat16)
                return carry

            lax.fori_loop(0, depth // width, compact, 0)
            if q == 0:
                @pl.when(k == tiles - 1)
                def _():
                    self_copy(k, q).start()

                @pl.when(k < tiles - 1)
                def _():
                    send_copy(k, q).start()
            else:
                send_copy(k, q).start()
        return carry

    lax.fori_loop(0, tiles, tile, 0)
    for k in range(tiles):
        for q in range(QUAD):
            if k == tiles - 1 and q == 0:
                self_copy(k, q).wait()
            else:
                if k >= tiles - 2:
                    send_copy(k, q).wait_send()
                send_copy(k, q).wait_recv()


def expert_exchange(n, cap_e, cap, rows, pick, pack, w1, w3, w2):
    local, depth, inner = w1.shape
    block = rows.shape[1]
    assert n % (2 * QUAD) == 0
    vmem = pl.BlockSpec(memory_space=pltpu.VMEM)
    anyspec = pl.BlockSpec(memory_space=pl.ANY)
    flops = 2 * n * local * cap_e * depth * inner * 3
    return pl.pallas_call(
        functools.partial(moe_kernel, n, cap_e, cap),
        out_shape=jax.ShapeDtypeStruct((n, cap, depth), jnp.bfloat16),
        in_specs=[anyspec, vmem, vmem, anyspec, anyspec, anyspec],
        out_specs=anyspec,
        scratch_shapes=[
            pltpu.VMEM(w1.shape, jnp.bfloat16),
            pltpu.VMEM(w3.shape, jnp.bfloat16),
            pltpu.VMEM(w2.shape, jnp.bfloat16),
            pltpu.VMEM((2, QUAD, block, depth), jnp.bfloat16),
            pltpu.VMEM((local, QUAD * cap_e, depth), jnp.bfloat16),
            pltpu.VMEM((QUAD * cap_e, inner), jnp.bfloat16),
            pltpu.VMEM((QUAD, local * cap_e, depth), jnp.bfloat16),
            pltpu.VMEM((2, QUAD, cap, depth), jnp.bfloat16),
            pltpu.SemaphoreType.DMA((3 * local,)),
            pltpu.SemaphoreType.DMA((2, QUAD)),
            pltpu.SemaphoreType.DMA((2, QUAD)),
            pltpu.SemaphoreType.DMA((n,)),
        ],
        compiler_params=pltpu.CompilerParams(collective_id=0, has_side_effects=True, vmem_limit_bytes=67_000_000),
        cost_estimate=pl.CostEstimate(flops=flops, bytes_accessed=80_000_000, transcendentals=0),
        name='moe_exchange',
    )(rows, pick, pack, w1, w3, w2)


def split3(x):
    hi = lax.reduce_precision(x, 8, 7)
    mid = lax.reduce_precision(x - hi, 8, 7)
    low = (x - hi) - mid
    return [part.astype(jnp.bfloat16) for part in (hi, mid, low)]


def solution(mesh):
    n = mesh.shape['ep']
    tok_spec = P(('dp', 'ep'), None)
    expert_spec = P('ep', None, None)

    def local_fn(hidden, norm_gain, w_gate, w1_shared, w3_shared, w2_shared, w1_experts, w3_experts, w2_experts, topk_ids):
        block, depth = hidden.shape
        local = w1_experts.shape[0]
        cap_e = block // 4
        cap = block * 3 // 8
        normed = rms_norm(hidden, norm_gain)
        all_rows = lax.all_gather(normed, 'ep', axis=0, tiled=True)
        all_ids = lax.all_gather(topk_ids, 'ep', axis=0, tiled=True)

        gate_probs = jax.nn.softmax(jnp.dot(normed, w_gate, preferred_element_type=jnp.float32), axis=-1)
        experts = jnp.arange(n * local)

        own_mask = jnp.any(topk_ids[:, :, None] == experts, axis=1).astype(jnp.float32)
        own_wts = (ROUTE_SCALE * gate_probs * own_mask).reshape(block, n, local)
        own_mask = own_mask.reshape(block, n, local)
        rank, _, _, start = assign_slots(own_mask, cap_e)
        slot = jnp.where((own_mask > 0) & (rank < cap_e), rank + start, -1.0)
        comb = jnp.sum(jnp.where(slot[:, :, :, None] == jnp.arange(cap, dtype=jnp.float32), own_wts[:, :, :, None], 0.0), axis=2)
        comb = comb.reshape(block, n * cap)
        comb3 = jnp.concatenate(split3(comb), axis=0)
        shared_out = swiglu(normed, w1_shared, w3_shared, w2_shared)

        ids_b = all_ids.reshape(n, block, -1)
        local_ids = lax.axis_index('ep') * local + jnp.arange(local)
        mask = jnp.any(ids_b[:, :, :, None] == local_ids, axis=2).astype(jnp.float32)
        rank_l, _, count_l, start_l = assign_slots(mask[:, :, None, :], cap_e)
        rank_l, count_l, start_l = rank_l[:, :, 0], count_l[:, 0], start_l[:, 0]
        place = jnp.arange(cap_e, dtype=jnp.float32)
        pick = ((mask.transpose(0, 2, 1)[:, :, None, :] > 0) & (rank_l.transpose(0, 2, 1)[:, :, None, :] == place[:, None]))
        pick = pick.astype(jnp.bfloat16).reshape(n, local * cap_e, block)
        pack = ((jnp.arange(cap, dtype=jnp.float32)[:, None, None] == start_l[:, None, :, None] + place) & (place < count_l[:, None, :, None]))
        pack = pack.astype(jnp.bfloat16).reshape(n, cap, local * cap_e)

        totals = jnp.sum(jnp.any(ids_b[:, :, :, None] == experts, axis=2).astype(jnp.float32), axis=1).reshape(n, n, local)
        over = jnp.any(totals > cap_e) | jnp.any(jnp.sum(jnp.minimum(totals, cap_e), axis=-1) > cap)

        pick, pack, comb3, shared_out = lax.optimization_barrier((pick, pack, comb3, shared_out))
        recv = expert_exchange(n, cap_e, cap, all_rows.reshape(n, block, depth), pick, pack, w1_experts, w3_experts, w2_experts)

        def correction(args):
            rows, row_ids, own_w, mask, rank_l, start_l, w1, w3, w2 = args
            wts = lax.all_gather(jnp.take_along_axis(own_w, topk_ids, axis=1), 'ep', axis=0, tiled=True)
            row_w = jnp.sum(jnp.where(row_ids[:, :, None] == local_ids, wts[:, :, None], 0.0), axis=1)
            left = (mask > 0) & ~((rank_l < cap_e) & (rank_l + start_l[:, None, :] < cap))
            row_w = jnp.where(left.reshape(n * block, local), row_w, 0.0)
            chunks = 16
            rows_c = rows.reshape(chunks, -1, depth)
            w_c = row_w.reshape(chunks, -1, local)

            def step(chunk):
                r, w = chunk
                acc = jnp.zeros(r.shape, jnp.float32)
                for e in range(local):
                    acc = acc + w[:, e:e + 1] * swiglu(r, w1[e], w3[e], w2[e]).astype(jnp.float32)
                return acc

            part = lax.map(step, (rows_c, w_c)).reshape(n * block, depth)
            return lax.psum_scatter(part, 'ep', scatter_dimension=0, tiled=True)

        extra = lax.cond(over, correction, lambda args: jnp.zeros((block, depth), jnp.float32),
                         (all_rows, all_ids, own_wts.reshape(block, n * local), mask, rank_l, start_l, w1_experts, w3_experts, w2_experts))
        parts = jnp.dot(comb3, recv.reshape(n * cap, depth), preferred_element_type=jnp.float32).reshape(3, block, depth)
        routed = parts[0] + (parts[1] + parts[2]) + extra
        return (hidden.astype(jnp.float32) + shared_out.astype(jnp.float32) + routed).astype(jnp.bfloat16)

    return jax.shard_map(local_fn, mesh=mesh, in_specs=(tok_spec, P(), P(), P(), P(), P(), expert_spec, expert_spec, expert_spec, tok_spec), out_specs=tok_spec, check_vma=False)
```

```python
import functools

import jax
import jax.numpy as jnp
from jax import lax
from jax.experimental import pallas as pl
from jax.experimental.pallas import tpu as pltpu
from jax.sharding import PartitionSpec as P

ROUTE_SCALE = 16
NORM_EPS = 1e-6
QUAD = 4
MESH = pl.DeviceIdType.MESH


def rms_norm(hidden, norm_gain):
    rows_f = hidden.astype(jnp.float32)
    inv_rms = lax.rsqrt(jnp.mean(rows_f * rows_f, axis=-1, keepdims=True) + NORM_EPS)
    return (rows_f * inv_rms * norm_gain.astype(jnp.float32)).astype(jnp.bfloat16)


def swiglu(rows_in, w_up, w_lin, w_down):
    gate_act = jnp.dot(rows_in, w_up, preferred_element_type=jnp.float32)
    lin_act = jnp.dot(rows_in, w_lin, preferred_element_type=jnp.float32)
    inner_act = (jax.nn.silu(gate_act) * lin_act).astype(jnp.bfloat16)
    return jnp.dot(inner_act, w_down, preferred_element_type=jnp.float32).astype(jnp.bfloat16)


def assign_slots(mask, cap_e):
    rows = mask.shape[-3]
    before = (jnp.arange(rows)[:, None] > jnp.arange(rows)[None, :]).astype(jnp.bfloat16)
    rank = jnp.einsum('ut,...tde->...ude', before, mask.astype(jnp.bfloat16), preferred_element_type=jnp.float32)
    total = jnp.sum(mask, axis=-3)
    count = jnp.minimum(total, cap_e)
    local = mask.shape[-1]
    later = (jnp.arange(local)[:, None] < jnp.arange(local)[None, :]).astype(jnp.float32)
    start = jnp.sum(count[..., :, None] * later, axis=-2)
    return rank, total, count, start


def flow_table(n):
    side = next(s for s in range(1, n + 1) if 2 * s * s >= n)
    flows = [(2, 2, 0), (2, 2, 1), (1, 3, 0), (3, 1, 0),
             (2, 0, 0), (2, 0, 1), (0, 2, 0), (0, 2, 1),
             (2, 1, 0), (2, 1, 1), (1, 2, 0), (1, 2, 1),
             (2, 3, 0), (2, 3, 1), (3, 2, 0), (3, 2, 1),
             (1, 0, 0), (3, 0, 0), (0, 1, 0), (0, 3, 0),
             (1, 0, 1), (3, 0, 1), (0, 1, 1), (0, 3, 1),
             (1, 1, 0), (3, 3, 0), (1, 1, 1), (3, 3, 1),
             (1, 3, 1), (3, 1, 1), (0, 0, 1), (0, 0, 0)]
    assert len(set(flows)) == n and side == 4
    relays = {}
    for i, (dx, dy, dc) in enumerate(flows):
        if 2 in (dx, dy):
            turn = 3 if dc else 1
            relays[i] = (turn if dx == 2 else 0, turn if dy == 2 else 0)
    return side, flows, relays


def device_at(me, side, step, sign=1):
    dx, dy, dc = step
    col, line = (me // 2) % side, me // (2 * side)
    col = (col + sign * dx + side) % side
    line = (line + sign * dy + side) % side
    return (line * side + col) * 2 + (me + dc) % 2


def moe_kernel(n, cap_e, cap, rows_ref, pick_ref, pack_ref, comb_ref, w1_ref, w3_ref, w2_ref,
               sum_ref, recv_ref, relay_ref,
               w1_v, w3_v, w2_v, row_v, xy_v, h_v, stage_v, w_sem, row_sem, send_sem, recv_sem, relay_sem, pass_sem, got_sem):
    side, flows, relays = flow_table(n)
    relay_slot = {i: j for j, i in enumerate(relays)}
    tiles = n // QUAD
    local, depth, inner = w1_ref.shape
    block = rows_ref.shape[1]
    me = lax.axis_index('ep')

    loads = []
    for e in range(local):
        for j, (src, dst) in enumerate(((w1_ref, w1_v), (w3_ref, w3_v), (w2_ref, w2_v))):
            loads.append(pltpu.make_async_copy(src.at[e], dst.at[e], w_sem.at[3 * e + j]))

    def row_start(t):
        for q in range(QUAD):
            peer = device_at(me, side, flows[t * QUAD + q])
            pltpu.make_async_copy(rows_ref.at[peer], row_v.at[t % 2, q], row_sem.at[t % 2, q]).start()

    def staged(t, q):
        return stage_v.at[t % 2, q]

    def send_copy(t, q):
        i = t * QUAD + q
        if i in relays:
            ax, ay = relays[i]
            j = relay_slot[i]
            dst, sem, to = relay_ref.at[j], relay_sem.at[j], device_at(me, side, (ax, ay, 0))
        else:
            dst, sem, to = recv_ref.at[i], recv_sem.at[i], device_at(me, side, flows[i])
        return pltpu.make_async_remote_copy(
            src_ref=staged(t, q), dst_ref=dst, send_sem=send_sem.at[t % 2, q], recv_sem=sem,
            device_id={'ep': to}, device_id_type=MESH)

    def pass_copy(i):
        (ax, ay), (dx, dy, dc), j = relays[i], flows[i], relay_slot[i]
        return pltpu.make_async_remote_copy(
            src_ref=relay_ref.at[j], dst_ref=recv_ref.at[i], send_sem=pass_sem.at[j], recv_sem=recv_sem.at[i],
            device_id={'ep': device_at(me, side, (dx - ax + side, dy - ay + side, dc))}, device_id_type=MESH)

    def self_copy(t, q):
        return pltpu.make_async_copy(staged(t, q), recv_ref.at[t * QUAD + q], recv_sem.at[t * QUAD + q])

    row_start(0)
    for load in loads:
        load.start()

    barrier = pltpu.get_barrier_semaphore()
    for off in range(1, n):
        pl.semaphore_signal(barrier, inc=1, device_id={'ep': (me + off) % n}, device_id_type=MESH)
    pl.semaphore_wait(barrier, n - 1)

    def columns(i, width):
        return pl.ds(pl.multiple_of(i * width, width), width)

    def tile(k, carry):
        slot = k % 2
        for t in range(tiles - 1):
            @pl.when(k == t)
            def _():
                row_start(t + 1)

        for q in range(QUAD):
            pltpu.make_async_copy(rows_ref.at[0], row_v.at[slot, q], row_sem.at[slot, q]).wait()
            width = min(512, depth)
            pick = pick_ref[k * QUAD + q]

            def gather(i, carry):
                got = jnp.dot(pick, row_v[slot, q, :, columns(i, width)], preferred_element_type=jnp.float32)
                got = got.astype(jnp.bfloat16)
                for e in range(local):
                    xy_v[e, q * cap_e:(q + 1) * cap_e, columns(i, width)] = got[e * cap_e:(e + 1) * cap_e]
                return carry

            lax.fori_loop(0, depth // width, gather, 0)

        for e in range(local):
            @pl.when(k == 0)
            def _():
                loads[3 * e].wait()
                loads[3 * e + 1].wait()

            def up_cols(at):
                rows_in = xy_v[e]
                gate_act = jnp.dot(rows_in, w1_v[e, :, at], preferred_element_type=jnp.float32)
                lin_act = jnp.dot(rows_in, w3_v[e, :, at], preferred_element_type=jnp.float32)
                h_v[:, at] = (jax.nn.silu(gate_act) * lin_act).astype(jnp.bfloat16)

            def up(i, carry):
                up_cols(columns(i, 256))
                return carry

            lax.fori_loop(0, inner // 256, up, 0)
            if inner % 256:
                up_cols(pl.ds(inner - inner % 256, inner % 256))

            @pl.when(k == 0)
            def _():
                loads[3 * e + 2].wait()

            def down(i, carry):
                at = columns(i, 256)
                got = jnp.dot(h_v[...], w2_v[e, :, at], preferred_element_type=jnp.float32).astype(jnp.bfloat16)
                for q in range(QUAD):
                    row = q * local * cap_e + e * cap_e
                    xy_v[local + row // (QUAD * cap_e), row % (QUAD * cap_e):row % (QUAD * cap_e) + cap_e, at] = got[q * cap_e:(q + 1) * cap_e]
                return carry

            lax.fori_loop(0, depth // 256, down, 0)

        for t in range(3, tiles):
            ready = [i for i in relays if i // QUAD == t - 3]
            if ready:
                @pl.when(k == t)
                def _():
                    for i in ready:
                        pltpu.make_async_copy(
                            relay_ref.at[relay_slot[i]], relay_ref.at[relay_slot[i]], relay_sem.at[relay_slot[i]]).wait()
                        pass_copy(i).start()

        @pl.when(k >= 2)
        def _():
            for q in range(QUAD):
                pltpu.make_async_copy(stage_v.at[slot, q], stage_v.at[slot, q], send_sem.at[slot, q]).wait()

        for q in range(QUAD):
            width = min(512, depth)
            pack = pack_ref[k * QUAD + q]
            row = q * local * cap_e

            def compact(i, carry):
                at = columns(i, width)
                y_in = xy_v[local + row // (QUAD * cap_e), row % (QUAD * cap_e):row % (QUAD * cap_e) + local * cap_e, at]
                got = jnp.dot(pack, y_in, preferred_element_type=jnp.float32)
                stage_v[slot, q, :, at] = got.astype(jnp.bfloat16)
                return carry

            lax.fori_loop(0, depth // width, compact, 0)

        for t in range(tiles):
            @pl.when(k == t)
            def _():
                for q in range(QUAD):
                    if flows[t * QUAD + q] == (0, 0, 0):
                        self_copy(t, q).start()
                    else:
                        send_copy(t, q).start()
        return carry

    lax.fori_loop(0, tiles, tile, 0)

    slots = 2 * local
    chunks = n // 2

    def got_copy(c, j):
        return pltpu.make_async_copy(recv_ref.at[2 * c + j], xy_v.at[c % slots, pl.ds(j * cap, cap), :], got_sem.at[c % slots, j])

    def add_chunk(c, first):
        for j in range(2):
            got_copy(c, j).wait()

        def add(i, carry):
            at = columns(i, 256)
            got = jnp.dot(comb_ref[c], xy_v[c % slots, :2 * cap, at], preferred_element_type=jnp.float32)
            got = got[:block] + (got[block:2 * block] + got[2 * block:])
            sum_ref[:, at] = got if first else sum_ref[:, at] + got
            return carry

        lax.fori_loop(0, depth // 256, add, 0)

    def fetch(c):
        for j in range(2):
            pltpu.make_async_copy(recv_ref.at[2 * c + j], recv_ref.at[2 * c + j], recv_sem.at[2 * c + j]).wait()
            got_copy(c, j).start()

    fetch(0)
    fetch(1)
    add_chunk(0, True)

    def step(c, carry):
        fetch(c + 1)
        add_chunk(c, False)
        return carry

    lax.fori_loop(1, chunks - 1, step, 0)
    add_chunk(chunks - 1, False)

    for i in relays:
        pltpu.make_async_copy(relay_ref.at[relay_slot[i]], relay_ref.at[relay_slot[i]], pass_sem.at[relay_slot[i]]).wait()
    for t in range(tiles - 2, tiles):
        for q in range(QUAD):
            if flows[t * QUAD + q] != (0, 0, 0):
                pltpu.make_async_copy(staged(t, q), staged(t, q), send_sem.at[t % 2, q]).wait()


def expert_exchange(n, cap_e, cap, rows, pick, pack, comb, w1, w3, w2):
    local, depth, inner = w1.shape
    block = rows.shape[1]
    assert n % (2 * QUAD) == 0 and block >= QUAD * cap_e and 2 * cap <= QUAD * cap_e and local * 2 == QUAD
    vmem = pl.BlockSpec(memory_space=pltpu.VMEM)
    anyspec = pl.BlockSpec(memory_space=pl.ANY)
    flops = 2 * n * local * cap_e * depth * inner * 3
    passing = len(flow_table(n)[2])
    return pl.pallas_call(
        functools.partial(moe_kernel, n, cap_e, cap),
        out_shape=(jax.ShapeDtypeStruct((block, depth), jnp.float32),
                   jax.ShapeDtypeStruct((n, cap, depth), jnp.bfloat16),
                   jax.ShapeDtypeStruct((passing, cap, depth), jnp.bfloat16)),
        in_specs=[anyspec, vmem, vmem, vmem, anyspec, anyspec, anyspec],
        out_specs=(vmem, anyspec, anyspec),
        scratch_shapes=[
            pltpu.VMEM(w1.shape, jnp.bfloat16),
            pltpu.VMEM(w3.shape, jnp.bfloat16),
            pltpu.VMEM(w2.shape, jnp.bfloat16),
            pltpu.VMEM((2, QUAD, block, depth), jnp.bfloat16),
            pltpu.VMEM((2 * local, QUAD * cap_e, depth), jnp.bfloat16),
            pltpu.VMEM((QUAD * cap_e, inner), jnp.bfloat16),
            pltpu.VMEM((2, QUAD, cap, depth), jnp.bfloat16),
            pltpu.SemaphoreType.DMA((3 * local,)),
            pltpu.SemaphoreType.DMA((2, QUAD)),
            pltpu.SemaphoreType.DMA((2, QUAD)),
            pltpu.SemaphoreType.DMA((n,)),
            pltpu.SemaphoreType.DMA((passing,)),
            pltpu.SemaphoreType.DMA((passing,)),
            pltpu.SemaphoreType.DMA((2 * local, 2)),
        ],
        compiler_params=pltpu.CompilerParams(collective_id=0, has_side_effects=True, vmem_limit_bytes=67_000_000),
        cost_estimate=pl.CostEstimate(flops=flops, bytes_accessed=80_000_000, transcendentals=0),
        name='moe_exchange',
    )(rows, pick, pack, comb, w1, w3, w2)[0]


def split3(x):
    hi = lax.reduce_precision(x, 8, 7)
    mid = lax.reduce_precision(x - hi, 8, 7)
    low = (x - hi) - mid
    return [part.astype(jnp.bfloat16) for part in (hi, mid, low)]


def solution(mesh):
    n = mesh.shape['ep']
    tok_spec = P(('dp', 'ep'), None)
    expert_spec = P('ep', None, None)

    def local_fn(hidden, norm_gain, w_gate, w1_shared, w3_shared, w2_shared, w1_experts, w3_experts, w2_experts, topk_ids):
        block, depth = hidden.shape
        local = w1_experts.shape[0]
        cap_e = block // 4
        cap = block * 3 // 8
        normed = rms_norm(hidden, norm_gain)
        all_rows = lax.all_gather(normed, 'ep', axis=0, tiled=True)
        all_ids = lax.all_gather(topk_ids, 'ep', axis=0, tiled=True)

        me = lax.axis_index('ep')
        side, flows, _ = flow_table(n)
        steps = tuple(jnp.array([flow[i] for flow in flows]) for i in range(3))
        dest = device_at(me, side, steps)
        src = device_at(me, side, steps, -1)
        experts = jnp.arange(n * local)
        from_experts = (src[:, None] * local + jnp.arange(local)).reshape(-1)

        gate_perm = jnp.dot(w_gate, (experts[:, None] == from_experts).astype(jnp.bfloat16), preferred_element_type=jnp.float32).astype(jnp.bfloat16)
        gate_probs = jax.nn.softmax(jnp.dot(normed, gate_perm, preferred_element_type=jnp.float32), axis=-1)
        own_mask = jnp.any(topk_ids[:, :, None] == from_experts, axis=1).astype(jnp.float32)
        own_wts = (ROUTE_SCALE * gate_probs * own_mask).reshape(block, n, local)
        own_mask = own_mask.reshape(block, n, local)
        rank, _, _, start = assign_slots(own_mask, cap_e)
        slot = jnp.where((own_mask > 0) & (rank < cap_e), rank + start, -1.0)
        slot, own_wts = slot.transpose(1, 2, 0), own_wts.transpose(1, 2, 0)
        comb = jnp.sum(jnp.where(slot[:, :, :, None] == jnp.arange(cap, dtype=jnp.float32), own_wts[:, :, :, None], 0.0), axis=1)
        comb = comb.reshape(n // 2, 2, block, cap).transpose(0, 2, 1, 3).reshape(n // 2, block, 2 * cap)
        comb3 = jnp.concatenate(split3(comb), axis=1)
        shared_out = swiglu(normed, w1_shared, w3_shared, w2_shared)

        order = (dest[:, None] == jnp.arange(n)).astype(jnp.bfloat16)
        ids_f = jnp.dot(order, all_ids.reshape(n, -1).astype(jnp.bfloat16), preferred_element_type=jnp.float32).reshape(n, block, -1)
        local_ids = me * local + jnp.arange(local)
        mask = jnp.any(ids_f[:, :, :, None] == local_ids.astype(jnp.float32), axis=2).astype(jnp.float32)
        rank_l, _, count_l, start_l = assign_slots(mask[:, :, None, :], cap_e)
        rank_l, count_l, start_l = rank_l[:, :, 0], count_l[:, 0], start_l[:, 0]
        place = jnp.arange(cap_e, dtype=jnp.float32)
        pick = ((mask.transpose(0, 2, 1)[:, :, None, :] > 0) & (rank_l.transpose(0, 2, 1)[:, :, None, :] == place[:, None]))
        pick = pick.astype(jnp.bfloat16).reshape(n, local * cap_e, block)
        pack = ((jnp.arange(cap, dtype=jnp.float32)[:, None, None] == start_l[:, None, :, None] + place) & (place < count_l[:, None, :, None]))
        pack = pack.astype(jnp.bfloat16).reshape(n, cap, local * cap_e)

        ids_b = all_ids.reshape(n, block, -1)
        totals = jnp.sum(jnp.any(ids_b[:, :, :, None] == experts, axis=2).astype(jnp.float32), axis=1).reshape(n, n, local)
        over = jnp.any(totals > cap_e) | jnp.any(jnp.sum(jnp.minimum(totals, cap_e), axis=-1) > cap)

        pick, pack, comb3, shared_out = lax.optimization_barrier((pick, pack, comb3, shared_out))
        routed = expert_exchange(n, cap_e, cap, all_rows.reshape(n, block, depth), pick, pack, comb3, w1_experts, w3_experts, w2_experts)

        def correction(rows, row_ids, w1, w3, w2):
            probs = jax.nn.softmax(jnp.dot(normed, w_gate, preferred_element_type=jnp.float32), axis=-1)
            wts = lax.all_gather(ROUTE_SCALE * jnp.take_along_axis(probs, topk_ids, axis=1), 'ep', axis=0, tiled=True)
            row_w = jnp.sum(jnp.where(row_ids[:, :, None] == local_ids, wts[:, :, None], 0.0), axis=1)
            mask = jnp.any(row_ids[:, :, None] == local_ids, axis=1).astype(jnp.float32).reshape(n, block, 1, local)
            rank, _, _, start = assign_slots(mask, cap_e)
            left = (mask > 0) & ~((rank < cap_e) & (rank + start[:, None] < cap))
            row_w = jnp.where(left.reshape(n * block, local), row_w, 0.0)
            chunks = 16

            def step(chunk):
                r, w = chunk
                acc = jnp.zeros(r.shape, jnp.float32)
                for e in range(local):
                    acc = acc + w[:, e:e + 1] * swiglu(r, w1[e], w3[e], w2[e]).astype(jnp.float32)
                return acc

            part = lax.map(step, (rows.reshape(chunks, -1, depth), row_w.reshape(chunks, -1, local))).reshape(n * block, depth)
            return lax.psum_scatter(part, 'ep', scatter_dimension=0, tiled=True)

        def finish(total):
            return (hidden.astype(jnp.float32) + shared_out.astype(jnp.float32) + total).astype(jnp.bfloat16)

        return lax.cond(over, lambda *args: finish(routed + correction(*args)), lambda *args: finish(routed),
                        all_rows, all_ids, w1_experts, w3_experts, w2_experts)

    return jax.shard_map(local_fn, mesh=mesh, in_specs=(tok_spec, P(), P(), P(), P(), P(), expert_spec, expert_spec, expert_spec, tok_spec), out_specs=tok_spec, check_vma=False)
```

```python
import functools

import jax
import jax.numpy as jnp
from jax import lax
from jax.experimental import pallas as pl
from jax.experimental.pallas import tpu as pltpu
from jax.sharding import PartitionSpec as P

ROUTE_SCALE = 16
NORM_EPS = 1e-6
QUAD = 4
MESH = pl.DeviceIdType.MESH


def rms_norm(hidden, norm_gain):
    rows_f = hidden.astype(jnp.float32)
    inv_rms = lax.rsqrt(jnp.mean(rows_f * rows_f, axis=-1, keepdims=True) + NORM_EPS)
    return (rows_f * inv_rms * norm_gain.astype(jnp.float32)).astype(jnp.bfloat16)


def swiglu(rows_in, w_up, w_lin, w_down):
    gate_act = jnp.dot(rows_in, w_up, preferred_element_type=jnp.float32)
    lin_act = jnp.dot(rows_in, w_lin, preferred_element_type=jnp.float32)
    inner_act = (jax.nn.silu(gate_act) * lin_act).astype(jnp.bfloat16)
    return jnp.dot(inner_act, w_down, preferred_element_type=jnp.float32).astype(jnp.bfloat16)


def assign_slots(mask, cap_e):
    rows = mask.shape[-3]
    before = (jnp.arange(rows)[:, None] > jnp.arange(rows)[None, :]).astype(jnp.bfloat16)
    rank = jnp.einsum('ut,...tde->...ude', before, mask.astype(jnp.bfloat16), preferred_element_type=jnp.float32)
    total = jnp.sum(mask, axis=-3)
    count = jnp.minimum(total, cap_e)
    local = mask.shape[-1]
    later = (jnp.arange(local)[:, None] < jnp.arange(local)[None, :]).astype(jnp.float32)
    start = jnp.sum(count[..., :, None] * later, axis=-2)
    return rank, total, count, start


def flow_table(n):
    side = next(s for s in range(1, n + 1) if 2 * s * s >= n)
    flows = [(2, 2, 0), (2, 2, 1), (1, 3, 0), (3, 1, 0),
             (2, 0, 0), (2, 0, 1), (0, 2, 0), (0, 2, 1),
             (2, 1, 0), (2, 1, 1), (1, 2, 0), (1, 2, 1),
             (2, 3, 0), (2, 3, 1), (3, 2, 0), (3, 2, 1),
             (1, 0, 0), (3, 0, 0), (0, 1, 0), (0, 3, 0),
             (1, 0, 1), (3, 0, 1), (0, 1, 1), (0, 3, 1),
             (1, 1, 0), (3, 3, 0), (1, 1, 1), (3, 3, 1),
             (1, 3, 1), (3, 1, 1), (0, 0, 1), (0, 0, 0)]
    assert len(set(flows)) == n and side == 4
    relays = {}
    for i, (dx, dy, dc) in enumerate(flows):
        if 2 in (dx, dy):
            turn = 3 if dc else 1
            relays[i] = (turn if dx == 2 else 0, turn if dy == 2 else 0)
    return side, flows, relays


def device_at(me, side, step, sign=1):
    dx, dy, dc = step
    col, line = (me // 2) % side, me // (2 * side)
    col = (col + sign * dx + side) % side
    line = (line + sign * dy + side) % side
    return (line * side + col) * 2 + (me + dc) % 2


def moe_kernel(n, cap_e, cap, rows_ref, pick_ref, pack_ref, comb_ref, w1_ref, w3_ref, w2_ref,
               sum_ref, recv_ref, relay_ref,
               w1_v, w3_v, wr_v, w2_v, row_v, xy_v, h_v, stage_v, w_sem, row_sem, send_sem, recv_sem, relay_sem, pass_sem, got_sem):
    side, flows, relays = flow_table(n)
    relay_slot = {i: j for j, i in enumerate(relays)}
    tiles = n // QUAD
    local, depth, inner = w1_ref.shape
    block = rows_ref.shape[1]
    me = lax.axis_index('ep')

    main = w1_v.shape[2]
    rest = inner - main

    def loads(e):
        whole, tail = pl.ds(0, main), pl.ds(main, rest)
        pairs = [(w1_ref.at[e, :, whole], w1_v.at[e]), (w3_ref.at[e, :, whole], w3_v.at[e])]
        if rest:
            pairs += [(w1_ref.at[e, :, tail], wr_v.at[e, :, pl.ds(0, rest)]), (w3_ref.at[e, :, tail], wr_v.at[e, :, pl.ds(rest, rest)])]
        pairs.append((w2_ref.at[e], w2_v.at[e]))
        return [pltpu.make_async_copy(src, dst, w_sem.at[e, j]) for j, (src, dst) in enumerate(pairs)]

    def row_start(t):
        for q in range(QUAD):
            peer = device_at(me, side, flows[t * QUAD + q])
            pltpu.make_async_copy(rows_ref.at[peer], row_v.at[t % 2, q], row_sem.at[t % 2, q]).start()

    def staged(t, q):
        return stage_v.at[t % 2, q]

    def send_copy(t, q):
        i = t * QUAD + q
        if i in relays:
            ax, ay = relays[i]
            j = relay_slot[i]
            dst, sem, to = relay_ref.at[j], relay_sem.at[j], device_at(me, side, (ax, ay, 0))
        else:
            dst, sem, to = recv_ref.at[i], recv_sem.at[i], device_at(me, side, flows[i])
        return pltpu.make_async_remote_copy(
            src_ref=staged(t, q), dst_ref=dst, send_sem=send_sem.at[t % 2, q], recv_sem=sem,
            device_id={'ep': to}, device_id_type=MESH)

    def pass_copy(i):
        (ax, ay), (dx, dy, dc), j = relays[i], flows[i], relay_slot[i]
        return pltpu.make_async_remote_copy(
            src_ref=relay_ref.at[j], dst_ref=recv_ref.at[i], send_sem=pass_sem.at[j], recv_sem=recv_sem.at[i],
            device_id={'ep': device_at(me, side, (dx - ax + side, dy - ay + side, dc))}, device_id_type=MESH)

    def self_copy(t, q):
        return pltpu.make_async_copy(staged(t, q), recv_ref.at[t * QUAD + q], recv_sem.at[t * QUAD + q])

    row_start(0)
    for load in loads(0):
        load.start()
    sum_ref[...] = jnp.zeros_like(sum_ref)

    barrier = pltpu.get_barrier_semaphore()
    for off in range(1, n):
        pl.semaphore_signal(barrier, inc=1, device_id={'ep': (me + off) % n}, device_id_type=MESH)
    pl.semaphore_wait(barrier, n - 1)

    def pieces(total, width):
        return [pl.ds(at, min(width, total - at)) for at in range(0, total, width)]

    def tile(k, carry):
        slot = k % 2
        for t in range(tiles - 1):
            @pl.when(k == t)
            def _():
                row_start(t + 1)

        for q in range(QUAD):
            pltpu.make_async_copy(rows_ref.at[0], row_v.at[slot, q], row_sem.at[slot, q]).wait()
            pick = pick_ref[k * QUAD + q]
            for at in pieces(depth, 512):
                got = jnp.dot(pick, row_v[slot, q, :, at], preferred_element_type=jnp.float32).astype(jnp.bfloat16)
                for e in range(local):
                    xy_v[e, q * cap_e:(q + 1) * cap_e, at] = got[e * cap_e:(e + 1) * cap_e]

        def expert(e, carry):
            @pl.when(k == 0)
            def _():
                for load in loads(e)[:-1]:
                    load.wait()

                @pl.when(e + 1 < local)
                def _():
                    for load in loads(e + 1):
                        load.start()

            rows_in = xy_v.at[e]
            for at in pieces(main, 256):
                gate_act = jnp.dot(rows_in[...], w1_v[e, :, at], preferred_element_type=jnp.float32)
                lin_act = jnp.dot(rows_in[...], w3_v[e, :, at], preferred_element_type=jnp.float32)
                h_v[:, at] = (jax.nn.silu(gate_act) * lin_act).astype(jnp.bfloat16)
            if rest:
                both = jnp.dot(rows_in[...], wr_v[e], preferred_element_type=jnp.float32)
                h_v[:, main:] = (jax.nn.silu(both[:, :rest]) * both[:, rest:]).astype(jnp.bfloat16)

            @pl.when(k == 0)
            def _():
                loads(e)[-1].wait()

            wide = min(1024, depth)

            def down(i, carry):
                for piece in pieces(wide, 256):
                    at = pl.ds(pl.multiple_of(i * wide + piece.start, 256), 256)
                    got = jnp.dot(h_v[...], w2_v[e, :, at], preferred_element_type=jnp.float32).astype(jnp.bfloat16)
                    for q in range(QUAD):
                        row = q * local * cap_e
                        xy_v[local + row // (QUAD * cap_e), pl.ds(pl.multiple_of(row % (QUAD * cap_e) + e * cap_e, cap_e), cap_e), at] = got[q * cap_e:(q + 1) * cap_e]
                return carry

            lax.fori_loop(0, depth // wide, down, 0)
            return carry

        lax.fori_loop(0, local, expert, 0)

        for t in range(3, tiles):
            ready = [i for i in relays if i // QUAD == t - 3]
            if ready:
                @pl.when(k == t)
                def _():
                    for i in ready:
                        pltpu.make_async_copy(
                            relay_ref.at[relay_slot[i]], relay_ref.at[relay_slot[i]], relay_sem.at[relay_slot[i]]).wait()
                        pass_copy(i).start()

        @pl.when(k >= 2)
        def _():
            for q in range(QUAD):
                pltpu.make_async_copy(stage_v.at[slot, q], stage_v.at[slot, q], send_sem.at[slot, q]).wait()

        for q in range(QUAD):
            pack = pack_ref[k * QUAD + q]
            row = q * local * cap_e
            for at in pieces(depth, 512):
                y_in = xy_v[local + row // (QUAD * cap_e), row % (QUAD * cap_e):row % (QUAD * cap_e) + local * cap_e, at]
                stage_v[slot, q, :, at] = jnp.dot(pack, y_in, preferred_element_type=jnp.float32).astype(jnp.bfloat16)

        for t in range(tiles):
            @pl.when(k == t)
            def _():
                for q in range(QUAD):
                    if flows[t * QUAD + q] == (0, 0, 0):
                        self_copy(t, q).start()
                    else:
                        send_copy(t, q).start()
        return carry

    lax.fori_loop(0, tiles, tile, 0)

    slots = 2 * local
    chunks = n // 2

    def got_copy(c, j):
        return pltpu.make_async_copy(recv_ref.at[2 * c + j], xy_v.at[c % slots, pl.ds(j * cap, cap), :], got_sem.at[c % slots, j])

    def fetch(c):
        for j in range(2):
            pltpu.make_async_copy(recv_ref.at[2 * c + j], recv_ref.at[2 * c + j], recv_sem.at[2 * c + j]).wait()
            got_copy(c, j).start()

    fetch(0)

    def add_chunk(c, carry):
        @pl.when(c + 1 < chunks)
        def _():
            fetch(c + 1)

        for j in range(2):
            got_copy(c, j).wait()
        for at in pieces(depth, 256):
            got = xy_v[c % slots, :2 * cap, at]
            parts = [jnp.dot(comb_ref[c, p * block:(p + 1) * block], got, preferred_element_type=jnp.float32) for p in range(3)]
            sum_ref[:, at] = sum_ref[:, at] + (parts[0] + parts[1] + parts[2])
        return carry

    lax.fori_loop(0, chunks, add_chunk, 0)

    for i in relays:
        pltpu.make_async_copy(relay_ref.at[relay_slot[i]], relay_ref.at[relay_slot[i]], pass_sem.at[relay_slot[i]]).wait()
    for t in range(tiles - 2, tiles):
        for q in range(QUAD):
            if flows[t * QUAD + q] != (0, 0, 0):
                pltpu.make_async_copy(staged(t, q), staged(t, q), send_sem.at[t % 2, q]).wait()


def expert_exchange(n, cap_e, cap, rows, pick, pack, comb, w1, w3, w2):
    local, depth, inner = w1.shape
    block = rows.shape[1]
    assert n % (2 * QUAD) == 0 and block >= QUAD * cap_e and 2 * cap <= QUAD * cap_e and local * 2 == QUAD
    vmem = pl.BlockSpec(memory_space=pltpu.VMEM)
    anyspec = pl.BlockSpec(memory_space=pl.ANY)
    flops = 2 * n * local * cap_e * depth * inner * 3
    passing = len(flow_table(n)[2])
    main = inner - inner % 256
    assert inner % 256 in (0, 128)
    return pl.pallas_call(
        functools.partial(moe_kernel, n, cap_e, cap),
        out_shape=(jax.ShapeDtypeStruct((block, depth), jnp.float32),
                   jax.ShapeDtypeStruct((n, cap, depth), jnp.bfloat16),
                   jax.ShapeDtypeStruct((passing, cap, depth), jnp.bfloat16)),
        in_specs=[anyspec, vmem, vmem, vmem, anyspec, anyspec, anyspec],
        out_specs=(vmem, anyspec, anyspec),
        scratch_shapes=[
            pltpu.VMEM((local, depth, main), jnp.bfloat16),
            pltpu.VMEM((local, depth, main), jnp.bfloat16),
            pltpu.VMEM((local, depth, max(256, 2 * (inner - main))), jnp.bfloat16),
            pltpu.VMEM(w2.shape, jnp.bfloat16),
            pltpu.VMEM((2, QUAD, block, depth), jnp.bfloat16),
            pltpu.VMEM((2 * local, QUAD * cap_e, depth), jnp.bfloat16),
            pltpu.VMEM((QUAD * cap_e, inner), jnp.bfloat16),
            pltpu.VMEM((2, QUAD, cap, depth), jnp.bfloat16),
            pltpu.SemaphoreType.DMA((local, 5)),
            pltpu.SemaphoreType.DMA((2, QUAD)),
            pltpu.SemaphoreType.DMA((2, QUAD)),
            pltpu.SemaphoreType.DMA((n,)),
            pltpu.SemaphoreType.DMA((passing,)),
            pltpu.SemaphoreType.DMA((passing,)),
            pltpu.SemaphoreType.DMA((2 * local, 2)),
        ],
        compiler_params=pltpu.CompilerParams(collective_id=0, has_side_effects=True, vmem_limit_bytes=67_000_000),
        cost_estimate=pl.CostEstimate(flops=flops, bytes_accessed=80_000_000, transcendentals=0),
        name='moe_exchange',
    )(rows, pick, pack, comb, w1, w3, w2)[0]


def split3(x):
    hi = lax.reduce_precision(x, 8, 7)
    mid = lax.reduce_precision(x - hi, 8, 7)
    low = (x - hi) - mid
    return [part.astype(jnp.bfloat16) for part in (hi, mid, low)]


def solution(mesh):
    n = mesh.shape['ep']
    tok_spec = P(('dp', 'ep'), None)
    expert_spec = P('ep', None, None)

    def local_fn(hidden, norm_gain, w_gate, w1_shared, w3_shared, w2_shared, w1_experts, w3_experts, w2_experts, topk_ids):
        block, depth = hidden.shape
        local = w1_experts.shape[0]
        cap_e = block // 4
        cap = block * 3 // 8
        normed = rms_norm(hidden, norm_gain)
        all_rows = lax.all_gather(normed, 'ep', axis=0, tiled=True)
        all_ids = lax.all_gather(topk_ids, 'ep', axis=0, tiled=True)

        me = lax.axis_index('ep')
        side, flows, _ = flow_table(n)
        steps = tuple(jnp.array([flow[i] for flow in flows]) for i in range(3))
        dest = device_at(me, side, steps)
        src = device_at(me, side, steps, -1)
        experts = jnp.arange(n * local)
        from_experts = (src[:, None] * local + jnp.arange(local)).reshape(-1)

        gate_perm = jnp.dot(w_gate, (experts[:, None] == from_experts).astype(jnp.bfloat16), preferred_element_type=jnp.float32).astype(jnp.bfloat16)
        gate_probs = jax.nn.softmax(jnp.dot(normed, gate_perm, preferred_element_type=jnp.float32), axis=-1)
        own_mask = jnp.any(topk_ids[:, :, None] == from_experts, axis=1).astype(jnp.float32)
        own_wts = (ROUTE_SCALE * gate_probs * own_mask).reshape(block, n, local)
        own_mask = own_mask.reshape(block, n, local)
        rank, _, _, start = assign_slots(own_mask, cap_e)
        slot = jnp.where((own_mask > 0) & (rank < cap_e), rank + start, -1.0)
        slot, own_wts = slot.transpose(1, 2, 0), own_wts.transpose(1, 2, 0)
        comb = jnp.sum(jnp.where(slot[:, :, :, None] == jnp.arange(cap, dtype=jnp.float32), own_wts[:, :, :, None], 0.0), axis=1)
        comb = comb.reshape(n // 2, 2, block, cap).transpose(0, 2, 1, 3).reshape(n // 2, block, 2 * cap)
        comb3 = jnp.concatenate(split3(comb), axis=1)
        shared_out = swiglu(normed, w1_shared, w3_shared, w2_shared)

        order = (dest[:, None] == jnp.arange(n)).astype(jnp.bfloat16)
        ids_f = jnp.dot(order, all_ids.reshape(n, -1).astype(jnp.bfloat16), preferred_element_type=jnp.float32).reshape(n, block, -1)
        local_ids = me * local + jnp.arange(local)
        mask = jnp.any(ids_f[:, :, :, None] == local_ids.astype(jnp.float32), axis=2).astype(jnp.float32)
        rank_l, _, count_l, start_l = assign_slots(mask[:, :, None, :], cap_e)
        rank_l, count_l, start_l = rank_l[:, :, 0], count_l[:, 0], start_l[:, 0]
        place = jnp.arange(cap_e, dtype=jnp.float32)
        pick = ((mask.transpose(0, 2, 1)[:, :, None, :] > 0) & (rank_l.transpose(0, 2, 1)[:, :, None, :] == place[:, None]))
        pick = pick.astype(jnp.bfloat16).reshape(n, local * cap_e, block)
        pack = ((jnp.arange(cap, dtype=jnp.float32)[:, None, None] == start_l[:, None, :, None] + place) & (place < count_l[:, None, :, None]))
        pack = pack.astype(jnp.bfloat16).reshape(n, cap, local * cap_e)

        ids_b = all_ids.reshape(n, block, -1)
        totals = jnp.sum(jnp.any(ids_b[:, :, :, None] == experts, axis=2).astype(jnp.float32), axis=1).reshape(n, n, local)
        over = jnp.any(totals > cap_e) | jnp.any(jnp.sum(jnp.minimum(totals, cap_e), axis=-1) > cap)

        pick, pack, comb3, shared_out = lax.optimization_barrier((pick, pack, comb3, shared_out))
        routed = expert_exchange(n, cap_e, cap, all_rows.reshape(n, block, depth), pick, pack, comb3, w1_experts, w3_experts, w2_experts)

        def correction(carry):
            total, todo = carry
            probs = jax.nn.softmax(jnp.dot(normed, w_gate, preferred_element_type=jnp.float32), axis=-1)
            wts = lax.all_gather(ROUTE_SCALE * jnp.take_along_axis(probs, topk_ids, axis=1), 'ep', axis=0, tiled=True)
            row_w = jnp.sum(jnp.where(all_ids[:, :, None] == local_ids, wts[:, :, None], 0.0), axis=1)
            mask = jnp.any(all_ids[:, :, None] == local_ids, axis=1).astype(jnp.float32).reshape(n, block, 1, local)
            rank, _, _, start = assign_slots(mask, cap_e)
            left = (mask > 0) & ~((rank < cap_e) & (rank + start[:, None] < cap))
            row_w = jnp.where(left.reshape(n * block, local), row_w, 0.0)
            chunks = 16

            def step(chunk):
                r, w = chunk
                acc = jnp.zeros(r.shape, jnp.float32)
                for e in range(local):
                    acc = acc + w[:, e:e + 1] * swiglu(r, w1_experts[e], w3_experts[e], w2_experts[e]).astype(jnp.float32)
                return acc

            part = lax.map(step, (all_rows.reshape(chunks, -1, depth), row_w.reshape(chunks, -1, local))).reshape(n * block, depth)
            return total + lax.psum_scatter(part, 'ep', scatter_dimension=0, tiled=True), jnp.logical_and(todo, False)

        routed = lax.while_loop(lambda carry: carry[1], correction, (routed, over))[0]
        return (hidden.astype(jnp.float32) + shared_out.astype(jnp.float32) + routed).astype(jnp.bfloat16)

    return jax.shard_map(local_fn, mesh=mesh, in_specs=(tok_spec, P(), P(), P(), P(), P(), expert_spec, expert_spec, expert_spec, tok_spec), out_specs=tok_spec, check_vma=False)
```

```python
import functools

import jax
import jax.numpy as jnp
from jax import lax
from jax.experimental import pallas as pl
from jax.experimental.pallas import tpu as pltpu
from jax.sharding import PartitionSpec as P

ROUTE_SCALE = 16
NORM_EPS = 1e-6
QUAD = 4
MESH = pl.DeviceIdType.MESH


def rms_norm(hidden, norm_gain):
    rows_f = hidden.astype(jnp.float32)
    inv_rms = lax.rsqrt(jnp.mean(rows_f * rows_f, axis=-1, keepdims=True) + NORM_EPS)
    return (rows_f * inv_rms * norm_gain.astype(jnp.float32)).astype(jnp.bfloat16)


def swiglu(rows_in, w_up, w_lin, w_down):
    gate_act = jnp.dot(rows_in, w_up, preferred_element_type=jnp.float32)
    lin_act = jnp.dot(rows_in, w_lin, preferred_element_type=jnp.float32)
    inner_act = (jax.nn.silu(gate_act) * lin_act).astype(jnp.bfloat16)
    return jnp.dot(inner_act, w_down, preferred_element_type=jnp.float32).astype(jnp.bfloat16)


def assign_slots(mask, cap_e):
    rows = mask.shape[-3]
    before = (jnp.arange(rows)[:, None] > jnp.arange(rows)[None, :]).astype(jnp.bfloat16)
    rank = jnp.einsum('ut,...tde->...ude', before, mask.astype(jnp.bfloat16), preferred_element_type=jnp.float32)
    total = jnp.sum(mask, axis=-3)
    count = jnp.minimum(total, cap_e)
    local = mask.shape[-1]
    later = (jnp.arange(local)[:, None] < jnp.arange(local)[None, :]).astype(jnp.float32)
    start = jnp.sum(count[..., :, None] * later, axis=-2)
    return rank, total, count, start


def flow_table(n):
    side = next(s for s in range(1, n + 1) if 2 * s * s >= n)
    flows = [(2, 2, 0), (2, 2, 1), (1, 3, 0), (3, 1, 0),
             (2, 1, 0), (2, 3, 0), (1, 2, 0), (3, 2, 0),
             (2, 1, 1), (2, 3, 1), (1, 2, 1), (3, 2, 1),
             (2, 0, 0), (2, 0, 1), (0, 2, 0), (0, 2, 1),
             (1, 1, 0), (3, 3, 0), (1, 1, 1), (3, 3, 1),
             (1, 3, 1), (3, 1, 1), (0, 1, 0), (0, 3, 0),
             (1, 0, 0), (3, 0, 0), (0, 1, 1), (0, 3, 1),
             (1, 0, 1), (3, 0, 1), (0, 0, 1), (0, 0, 0)]
    assert len(set(flows)) == n and side == 4
    return side, flows


def device_at(me, side, step, sign=1):
    dx, dy, dc = step
    col, line = (me // 2) % side, me // (2 * side)
    col = (col + sign * dx + side) % side
    line = (line + sign * dy + side) % side
    return (line * side + col) * 2 + (me + dc) % 2


def moe_kernel(n, cap_e, cap, rows_ref, pick_ref, pack_ref, comb_hbm, w1_ref, w3_ref, w2_ref,
               sum_ref, recv_ref,
               w1_v, w3_v, wr_v, w2_v, row_v, xy_v, h_v, stage_v, comb_ref, w_sem, row_sem, send_sem, recv_sem, got_sem, comb_sem):
    side, flows = flow_table(n)
    tiles = n // QUAD
    local, depth, inner = w1_ref.shape
    block = rows_ref.shape[1]
    me = lax.axis_index('ep')

    main = w1_v.shape[2]
    rest = inner - main

    def loads(e):
        whole, tail = pl.ds(0, main), pl.ds(main, rest)
        pairs = [(w1_ref.at[e, :, whole], w1_v.at[e]), (w3_ref.at[e, :, whole], w3_v.at[e])]
        if rest:
            pairs += [(w1_ref.at[e, :, tail], wr_v.at[e, :, pl.ds(0, rest)]), (w3_ref.at[e, :, tail], wr_v.at[e, :, pl.ds(rest, rest)])]
        pairs.append((w2_ref.at[e], w2_v.at[e]))
        return [pltpu.make_async_copy(src, dst, w_sem.at[e, j]) for j, (src, dst) in enumerate(pairs)]

    def row_start(t):
        for q in range(QUAD):
            peer = device_at(me, side, flows[t * QUAD + q])
            pltpu.make_async_copy(rows_ref.at[peer], row_v.at[t % 2, q], row_sem.at[t % 2, q]).start()

    def staged(t, q):
        return stage_v.at[t % 2, q]

    def send_copy(t, q):
        i = t * QUAD + q
        return pltpu.make_async_remote_copy(
            src_ref=staged(t, q), dst_ref=recv_ref.at[i], send_sem=send_sem.at[t % 2, q], recv_sem=recv_sem.at[i],
            device_id={'ep': device_at(me, side, flows[i])}, device_id_type=MESH)

    def self_copy(t, q):
        return pltpu.make_async_copy(staged(t, q), recv_ref.at[t * QUAD + q], recv_sem.at[t * QUAD + q])

    row_start(0)
    for load in loads(0):
        load.start()
    sum_ref[...] = jnp.zeros_like(sum_ref)

    barrier = pltpu.get_barrier_semaphore()
    for off in range(1, n):
        pl.semaphore_signal(barrier, inc=1, device_id={'ep': (me + off) % n}, device_id_type=MESH)
    pl.semaphore_wait(barrier, n - 1)

    def pieces(total, width):
        return [pl.ds(at, min(width, total - at)) for at in range(0, total, width)]

    def tile(k, carry):
        slot = k % 2
        for t in range(tiles - 1):
            @pl.when(k == t)
            def _():
                row_start(t + 1)

        for q in range(QUAD):
            pltpu.make_async_copy(rows_ref.at[0], row_v.at[slot, q], row_sem.at[slot, q]).wait()
            pick = pick_ref[k * QUAD + q]
            for at in pieces(depth, 512):
                got = jnp.dot(pick, row_v[slot, q, :, at], preferred_element_type=jnp.float32).astype(jnp.bfloat16)
                for e in range(local):
                    xy_v[e, q * cap_e:(q + 1) * cap_e, at] = got[e * cap_e:(e + 1) * cap_e]

        @pl.when(k == 2)
        def _():
            pltpu.make_async_copy(comb_hbm, comb_ref, comb_sem).start()

        def expert(e, carry):
            @pl.when(k == 0)
            def _():
                for load in loads(e)[:-1]:
                    load.wait()

                @pl.when(e + 1 < local)
                def _():
                    for load in loads(e + 1):
                        load.start()

            rows_in = xy_v.at[e]
            for at in pieces(main, 256):
                gate_act = jnp.dot(rows_in[...], w1_v[e, :, at], preferred_element_type=jnp.float32)
                lin_act = jnp.dot(rows_in[...], w3_v[e, :, at], preferred_element_type=jnp.float32)
                h_v[:, at] = (jax.nn.silu(gate_act) * lin_act).astype(jnp.bfloat16)
            if rest:
                both = jnp.dot(rows_in[...], wr_v[e], preferred_element_type=jnp.float32)
                h_v[:, main:] = (jax.nn.silu(both[:, :rest]) * both[:, rest:]).astype(jnp.bfloat16)

            @pl.when(k == 0)
            def _():
                loads(e)[-1].wait()

            wide = min(1024, depth)

            def down(i, carry):
                for piece in pieces(wide, 256):
                    at = pl.ds(pl.multiple_of(i * wide + piece.start, 256), 256)
                    got = jnp.dot(h_v[...], w2_v[e, :, at], preferred_element_type=jnp.float32).astype(jnp.bfloat16)
                    for q in range(QUAD):
                        row = q * local * cap_e
                        xy_v[local + row // (QUAD * cap_e), pl.ds(pl.multiple_of(row % (QUAD * cap_e) + e * cap_e, cap_e), cap_e), at] = got[q * cap_e:(q + 1) * cap_e]
                return carry

            lax.fori_loop(0, depth // wide, down, 0)
            return carry

        lax.fori_loop(0, local, expert, 0)

        @pl.when(k >= 2)
        def _():
            for q in range(QUAD):
                pltpu.make_async_copy(stage_v.at[slot, q], stage_v.at[slot, q], send_sem.at[slot, q]).wait()

        for q in range(QUAD):
            pack = pack_ref[k * QUAD + q]
            row = q * local * cap_e
            for at in pieces(depth, 512):
                y_in = xy_v[local + row // (QUAD * cap_e), row % (QUAD * cap_e):row % (QUAD * cap_e) + local * cap_e, at]
                stage_v[slot, q, :, at] = jnp.dot(pack, y_in, preferred_element_type=jnp.float32).astype(jnp.bfloat16)

        for t in range(tiles):
            @pl.when(k == t)
            def _():
                for q in range(QUAD):
                    if flows[t * QUAD + q] == (0, 0, 0):
                        self_copy(t, q).start()
                    else:
                        send_copy(t, q).start()
        return carry

    lax.fori_loop(0, tiles, tile, 0)

    pltpu.make_async_copy(comb_hbm, comb_ref, comb_sem).wait()

    slots = 2 * local
    chunks = n // 2

    def got_copy(c, j):
        return pltpu.make_async_copy(recv_ref.at[2 * c + j], xy_v.at[c % slots, pl.ds(j * cap, cap), :], got_sem.at[c % slots, j])

    def fetch(c):
        for j in range(2):
            pltpu.make_async_copy(recv_ref.at[2 * c + j], recv_ref.at[2 * c + j], recv_sem.at[2 * c + j]).wait()
            got_copy(c, j).start()

    fetch(0)

    def add_chunk(c, carry):
        @pl.when(c + 1 < chunks)
        def _():
            fetch(c + 1)

        for j in range(2):
            got_copy(c, j).wait()
        for at in pieces(depth, 256):
            got = xy_v[c % slots, :2 * cap, at]
            parts = [jnp.dot(comb_ref[c, p * block:(p + 1) * block], got, preferred_element_type=jnp.float32) for p in range(3)]
            sum_ref[:, at] = sum_ref[:, at] + (parts[0] + parts[1] + parts[2])
        return carry

    lax.fori_loop(0, chunks, add_chunk, 0)

    for t in range(tiles - 2, tiles):
        for q in range(QUAD):
            if flows[t * QUAD + q] != (0, 0, 0):
                pltpu.make_async_copy(staged(t, q), staged(t, q), send_sem.at[t % 2, q]).wait()


def expert_exchange(n, cap_e, cap, rows, pick, pack, comb, w1, w3, w2):
    local, depth, inner = w1.shape
    block = rows.shape[1]
    assert n % (2 * QUAD) == 0 and block >= QUAD * cap_e and 2 * cap <= QUAD * cap_e and local * 2 == QUAD
    vmem = pl.BlockSpec(memory_space=pltpu.VMEM)
    anyspec = pl.BlockSpec(memory_space=pl.ANY)
    flops = 2 * n * local * cap_e * depth * inner * 3
    main = inner - inner % 256
    assert inner % 256 in (0, 128)
    return pl.pallas_call(
        functools.partial(moe_kernel, n, cap_e, cap),
        out_shape=(jax.ShapeDtypeStruct((block, depth), jnp.float32),
                   jax.ShapeDtypeStruct((n, cap, depth), jnp.bfloat16)),
        in_specs=[anyspec, vmem, vmem, anyspec, anyspec, anyspec, anyspec],
        out_specs=(vmem, anyspec),
        scratch_shapes=[
            pltpu.VMEM((local, depth, main), jnp.bfloat16),
            pltpu.VMEM((local, depth, main), jnp.bfloat16),
            pltpu.VMEM((local, depth, max(256, 2 * (inner - main))), jnp.bfloat16),
            pltpu.VMEM(w2.shape, jnp.bfloat16),
            pltpu.VMEM((2, QUAD, block, depth), jnp.bfloat16),
            pltpu.VMEM((2 * local, QUAD * cap_e, depth), jnp.bfloat16),
            pltpu.VMEM((QUAD * cap_e, inner), jnp.bfloat16),
            pltpu.VMEM((2, QUAD, cap, depth), jnp.bfloat16),
            pltpu.VMEM(comb.shape, jnp.bfloat16),
            pltpu.SemaphoreType.DMA((local, 5)),
            pltpu.SemaphoreType.DMA((2, QUAD)),
            pltpu.SemaphoreType.DMA((2, QUAD)),
            pltpu.SemaphoreType.DMA((n,)),
            pltpu.SemaphoreType.DMA((2 * local, 2)),
            pltpu.SemaphoreType.DMA,
        ],
        compiler_params=pltpu.CompilerParams(collective_id=0, has_side_effects=True, vmem_limit_bytes=67_000_000),
        cost_estimate=pl.CostEstimate(flops=flops, bytes_accessed=80_000_000, transcendentals=0),
        name='moe_exchange',
    )(rows, pick, pack, comb, w1, w3, w2)[0]


def split3(x):
    hi = lax.reduce_precision(x, 8, 7)
    mid = lax.reduce_precision(x - hi, 8, 7)
    low = (x - hi) - mid
    return [part.astype(jnp.bfloat16) for part in (hi, mid, low)]


def solution(mesh):
    n = mesh.shape['ep']
    tok_spec = P(('dp', 'ep'), None)
    expert_spec = P('ep', None, None)

    def local_fn(hidden, norm_gain, w_gate, w1_shared, w3_shared, w2_shared, w1_experts, w3_experts, w2_experts, topk_ids):
        block, depth = hidden.shape
        local = w1_experts.shape[0]
        cap_e = block // 4
        cap = block * 3 // 8
        normed = rms_norm(hidden, norm_gain)
        all_rows = lax.all_gather(normed, 'ep', axis=0, tiled=True)
        all_ids = lax.all_gather(topk_ids, 'ep', axis=0, tiled=True)

        me = lax.axis_index('ep')
        side, flows = flow_table(n)
        steps = tuple(jnp.array([flow[i] for flow in flows]) for i in range(3))
        dest = device_at(me, side, steps)
        src = device_at(me, side, steps, -1)
        experts = jnp.arange(n * local)
        from_experts = (src[:, None] * local + jnp.arange(local)).reshape(-1)

        gate_perm = jnp.dot(w_gate, (experts[:, None] == from_experts).astype(jnp.bfloat16), preferred_element_type=jnp.float32).astype(jnp.bfloat16)
        gate_probs = jax.nn.softmax(jnp.dot(normed, gate_perm, preferred_element_type=jnp.float32), axis=-1)
        own_mask = jnp.any(topk_ids[:, :, None] == from_experts, axis=1).astype(jnp.float32)
        own_wts = (ROUTE_SCALE * gate_probs * own_mask).reshape(block, n, local)
        own_mask = own_mask.reshape(block, n, local)
        rank, _, _, start = assign_slots(own_mask, cap_e)
        slot = jnp.where((own_mask > 0) & (rank < cap_e), rank + start, -1.0)
        slot, own_wts = slot.transpose(1, 2, 0), own_wts.transpose(1, 2, 0)
        comb = jnp.sum(jnp.where(slot[:, :, :, None] == jnp.arange(cap, dtype=jnp.float32), own_wts[:, :, :, None], 0.0), axis=1)
        comb = comb.reshape(n // 2, 2, block, cap).transpose(0, 2, 1, 3).reshape(n // 2, block, 2 * cap)
        comb3 = jnp.concatenate(split3(comb), axis=1)
        shared_out = swiglu(normed, w1_shared, w3_shared, w2_shared)

        order = (dest[:, None] == jnp.arange(n)).astype(jnp.bfloat16)
        ids_f = jnp.dot(order, all_ids.reshape(n, -1).astype(jnp.bfloat16), preferred_element_type=jnp.float32).reshape(n, block, -1)
        local_ids = me * local + jnp.arange(local)
        mask = jnp.any(ids_f[:, :, :, None] == local_ids.astype(jnp.float32), axis=2).astype(jnp.float32)
        rank_l, _, count_l, start_l = assign_slots(mask[:, :, None, :], cap_e)
        rank_l, count_l, start_l = rank_l[:, :, 0], count_l[:, 0], start_l[:, 0]
        place = jnp.arange(cap_e, dtype=jnp.float32)
        pick = ((mask.transpose(0, 2, 1)[:, :, None, :] > 0) & (rank_l.transpose(0, 2, 1)[:, :, None, :] == place[:, None]))
        pick = pick.astype(jnp.bfloat16).reshape(n, local * cap_e, block)
        pack = ((jnp.arange(cap, dtype=jnp.float32)[:, None, None] == start_l[:, None, :, None] + place) & (place < count_l[:, None, :, None]))
        pack = pack.astype(jnp.bfloat16).reshape(n, cap, local * cap_e)

        ids_b = all_ids.reshape(n, block, -1)
        totals = jnp.sum(jnp.any(ids_b[:, :, :, None] == experts, axis=2).astype(jnp.float32), axis=1).reshape(n, n, local)
        over = jnp.any(totals > cap_e) | jnp.any(jnp.sum(jnp.minimum(totals, cap_e), axis=-1) > cap)

        pick, pack, comb3, shared_out = lax.optimization_barrier((pick, pack, comb3, shared_out))
        routed = expert_exchange(n, cap_e, cap, all_rows.reshape(n, block, depth), pick, pack, comb3, w1_experts, w3_experts, w2_experts)

        def correction(carry):
            total, todo = carry
            probs = jax.nn.softmax(jnp.dot(normed, w_gate, preferred_element_type=jnp.float32), axis=-1)
            wts = lax.all_gather(ROUTE_SCALE * jnp.take_along_axis(probs, topk_ids, axis=1), 'ep', axis=0, tiled=True)
            row_w = jnp.sum(jnp.where(all_ids[:, :, None] == local_ids, wts[:, :, None], 0.0), axis=1)
            mask = jnp.any(all_ids[:, :, None] == local_ids, axis=1).astype(jnp.float32).reshape(n, block, 1, local)
            rank, _, _, start = assign_slots(mask, cap_e)
            left = (mask > 0) & ~((rank < cap_e) & (rank + start[:, None] < cap))
            row_w = jnp.where(left.reshape(n * block, local), row_w, 0.0)
            chunks = n * block // 128

            def step(i, part):
                e, at = i % local, (i // local) * (n * block // chunks)
                got = swiglu(lax.dynamic_slice_in_dim(all_rows, at, n * block // chunks), w1_experts[e], w3_experts[e], w2_experts[e])
                wts = jnp.sum(jnp.where(jnp.arange(local) == e, lax.dynamic_slice_in_dim(row_w, at, n * block // chunks), 0.0), axis=1)
                old = lax.dynamic_slice_in_dim(part, at, n * block // chunks)
                return lax.dynamic_update_slice_in_dim(part, old + wts[:, None] * got.astype(jnp.float32), at, axis=0)

            part = lax.fori_loop(0, chunks * local, step, jnp.zeros((n * block, depth), jnp.float32))
            part = part.reshape(n, block, depth)
            ring = [(i, (i + 1) % n) for i in range(n)]

            def hop(i, acc):
                return lax.ppermute(acc, 'ep', ring) + part[(me - 2 - i + 2 * n) % n]

            return total + lax.fori_loop(0, n - 1, hop, part[(me - 1 + n) % n]), jnp.logical_and(todo, False)

        routed = lax.while_loop(lambda carry: carry[1], correction, (routed, over))[0]
        return (hidden.astype(jnp.float32) + shared_out.astype(jnp.float32) + routed).astype(jnp.bfloat16)

    return jax.shard_map(local_fn, mesh=mesh, in_specs=(tok_spec, P(), P(), P(), P(), P(), expert_spec, expert_spec, expert_spec, tok_spec), out_specs=tok_spec, check_vma=False)
```
